32 devices in a mesh: ga: 1, ea: 32 (over z, y, x, core).
Axes of the slice: x: 2, y: 2, z: 4, core: 2. Of those that a mesh axis runs over, the one named last changes fastest.
Arguments:
- tokens: bfloat16 [256, 7168], P(('ga', 'ea')), may hold values from -6 to 6
- route_slot: int32 [256, 2], P(('ga', 'ea')), may hold values from 0 to 3, all different within a row; in each aligned block of 8 rows (0 to 7, 8 to 15, ...) at most 8 rows name the same one
- gates: float32 [256, 2], P(('ga', 'ea')), may hold values from 0.2 to 1
- gate_up: bfloat16 [32, 7168, 512], P('ea'), may hold values from -0.0625 to 0.0625
- down: bfloat16 [32, 256, 7168], P('ea'), may hold values from -0.125 to 0.125
Outputs:
- mixed: bfloat16 [256, 7168], P(('ga', 'ea'))
The draws below stay inside these ranges and needn't reach their ends.
Inputs may be any that keep to these rules, and one draw needn't show every extreme that they name: `route_slot`: each token names 2 different replicas. Among the tokens of one device no replica is named more than 8 times, and some device names some replica exactly 8 times.
All inputs are finite; a program needn't handle non-finite values.
Results may differ from the reference program's by a relative error of at most 0.0087.
Values may be sent and summed in bfloat16 or wider, within the bound.
A program may use at most 64 MiB of HBM per device.

```python
import math
import jax
import jax.numpy as jnp
import numpy as np
from jax import lax

D = 7168
FF = 2048
TP = 8
TOPK = 2
TOK_DEV = 8
HS = 256
SLOTS = 4
CAP = 8
TOKENS = 256
N_EA = 32


def levels(own_key, shape, cuts, smallest, high):
    loudness = 1.0
    for dim, shards_of in cuts:
        heights = jax.random.uniform(jax.random.fold_in(jax.random.fold_in(own_key, 6), dim), (shards_of,), jnp.float32, smallest / len(cuts), high / len(cuts))
        loudness = loudness * jnp.repeat(jnp.exp(heights), shape[dim] // shards_of).reshape((-1,) + (1,) * (len(shape) - 1 - dim))
    return loudness


def routed_block(own_key, own, number, rows, number_of, top, reach, slope):
    sequence = jax.random.permutation(own_key, number_of)
    crowded, ordinary = shares(number_of, rows * top, reach, slope, True), shares(number_of, rows * top, reach, slope, False)
    places = jnp.arange(number_of)

    def named(sizes, offset_by):
        used = int((sizes > 0).sum())
        fixed = max(1, used // 4)
        passed = fixed + (places - fixed + offset_by * (used - fixed)) % max(1, number_of - fixed)
        return jnp.zeros((number_of,), jnp.int32).at[sequence[jnp.where(places < fixed, places, passed)]].set(jnp.asarray(sizes, jnp.int32))

    sizes = jnp.where(number % 4 == 0, named(crowded, number // 4), named(ordinary, number - number // 4 - 1))
    mixed = jax.random.permutation(jax.random.fold_in(own, 3), number_of)
    donor, receiver = mixed[0:number_of // 2 * 2:2], mixed[1:number_of // 2 * 2:2]
    slack = jnp.minimum(sizes[donor] - 1, reach - sizes[receiver]) // 2
    slack = jnp.where((donor == sequence[0]) | (receiver == sequence[0]) | (sizes[receiver] == 0), 0, jnp.maximum(slack, 0))
    passed = jax.random.randint(jax.random.fold_in(own, 4), (number_of // 2,), 0, 1 << 20) % (slack + 1)
    sizes = sizes.at[donor].add(-passed).at[receiver].add(passed)
    items = jnp.searchsorted(jnp.cumsum(sizes), jnp.arange(rows * top), side="right").astype(jnp.int32)
    grid = items.reshape(top, rows).T
    grid = grid[jax.random.permutation(jax.random.fold_in(own, 1), rows)]
    offset_by = jax.random.randint(jax.random.fold_in(own, 2), (rows, 1), 0, top)
    return jnp.take_along_axis(grid, (jnp.arange(top)[None, :] + offset_by) % top, axis=1)


def shares(number_of, total, bound, slope, full):
    weights = [(1 << 20) // math.isqrt(standing ** slope) + 1 for standing in range(1, number_of + 1)]
    largest = bound if full else min(bound, max(-(-total // number_of), total * weights[0] // sum(weights)))
    least = 1 if total - largest >= number_of - 1 else 0
    given, surplus = [largest] + [least] * (number_of - 1), total - largest - least * (number_of - 1)
    while surplus > 0:
        candidates = [i for i in range(1, number_of) if given[i] < largest] or [i for i in range(1, number_of) if given[i] < bound]
        mass, left = sum([weights[i] for i in candidates]), surplus
        for i in candidates:
            more = min(bound - given[i], max(1, left * weights[i] // mass), surplus)
            given[i] = given[i] + more
            surplus = surplus - more
    return np.array(given)


def normal_values(rng, extent, spread, limit, cuts=(), held_as=jnp.bfloat16):
    loudness = levels(rng, extent, cuts, -0.22, 0.18) if cuts else 1.0
    values = jax.random.normal(rng, extent, jnp.float32) * spread * loudness
    return jnp.minimum(jnp.maximum(values, -limit), limit).astype(held_as)


def setup_inputs(seed: int = 0, part: int = 0) -> dict:
    key_of = jax.random.split(jax.random.key(seed), 6)
    part_splits = jax.random.split(jax.random.fold_in(key_of[5], part), 6)
    tokens = normal_values(part_splits[0], (TOKENS, D), 1.0, 6.0, ((0, 32),))
    route_slot_keys = jax.random.split(jax.random.fold_in(part_splits[1], 1), TOKENS // TOK_DEV)
    route_slot_turns = jax.random.permutation(jax.random.fold_in(part_splits[1], 3), TOKENS // TOK_DEV)
    route_slot = jax.vmap(lambda own, number: routed_block(jax.random.fold_in(part_splits[1], 2), own, number, TOK_DEV, SLOTS, TOPK, CAP, 2))(route_slot_keys, route_slot_turns).reshape((TOKENS, TOPK))
    gates = jnp.clip(0.2 + 0.8 * jax.random.uniform(part_splits[2], (TOKENS, TOPK), jnp.float32) ** levels(part_splits[2], (TOKENS, TOPK), ((0, 32),), -0.2, 0.2), 0.2, 1.0)
    gate_up = normal_values(key_of[3], (N_EA, D, 2 * HS), D ** -0.5, 0.0625, ((0, 32),))
    down = normal_values(key_of[4], (N_EA, HS, D), FF ** -0.5, 0.125, ((0, 32),))
    return {"tokens": tokens, "route_slot": route_slot, "gates": gates, "gate_up": gate_up, "down": down}


def reference(tokens, route_slot, gates, gate_up, down):
    pairs = TOKENS * TOPK
    flat_slot = route_slot.reshape(-1).astype(jnp.int32)
    flat_gate = gates.reshape(-1)
    owner = (jnp.arange(pairs, dtype=jnp.int32) // TOPK).astype(jnp.int32)
    order = jnp.argsort(flat_slot, stable=True).astype(jnp.int32)
    counts = jnp.sum((flat_slot[:, None] == jnp.arange(SLOTS, dtype=jnp.int32)[None, :]).astype(jnp.int32), axis=0)
    starts = (jnp.cumsum(counts) - counts).astype(jnp.int32)
    most_rows = N_EA * CAP

    def one_slot(total, slot):
        begin = jnp.minimum(starts[slot], pairs - most_rows).astype(jnp.int32)
        picked = lax.dynamic_slice_in_dim(order, begin, most_rows, 0)
        member = (flat_slot[picked] == slot)
        rows = tokens[owner[picked]]
        blocks = lax.dynamic_slice_in_dim(gate_up, (slot * TP).astype(jnp.int32), TP, 0)
        wide = jnp.transpose(blocks, (1, 0, 2)).reshape(D, TP * 2 * HS)
        both = jnp.dot(rows, wide, preferred_element_type=jnp.float32).reshape(most_rows, TP, 2 * HS)
        hidden = (jax.nn.silu(both[:, :, :HS]) * both[:, :, HS:]).astype(jnp.bfloat16).reshape(most_rows, FF)
        downs = lax.dynamic_slice_in_dim(down, (slot * TP).astype(jnp.int32), TP, 0).reshape(FF, D)
        result = jnp.dot(hidden, downs, preferred_element_type=jnp.float32)
        weight = jnp.where(member, flat_gate[picked], jnp.float32(0.0))
        total = total.at[owner[picked]].add(result * weight[:, None])
        return total, None

    total, unused = lax.scan(one_slot, jnp.zeros((TOKENS, D), jnp.float32), jnp.arange(SLOTS, dtype=jnp.int32))
    return total.astype(jnp.bfloat16)
```

```python
import functools

import jax
import jax.numpy as jnp
from jax import lax
from jax.experimental import pallas as pl
from jax.experimental.pallas import tpu as pltpu
from jax.sharding import PartitionSpec as P

TP = 8
LANES = 128
F32 = jnp.float32
BF16 = jnp.bfloat16


def chunk_count(width):
    return next(k for k in (7, 4, 2, 1) if width % (k * 2 * LANES) == 0)


def copies_per_launch(outer, chunks):
    return chunks * ((outer - 1) + 8 + 5 + (outer - 1))


def kernel(outer, chunks, *refs):
    tokens, route, gates, gate_up, down, out = refs[:6]
    at = 6

    def take(count):
        nonlocal at
        at += count
        return refs[at - count : at]

    zin, xin = take(chunks), take(chunks)
    part, from_core = take(chunks), take(chunks)
    a_sum, b_sum, a_one, b_one = take(chunks), take(chunks), take(chunks), take(chunks)
    a_mid, b_mid, a_two, b_two = take(chunks), take(chunks), take(chunks), take(chunks)
    z_send, z_recv = take(chunks), take(chunks)
    w_in, w_out, both, send_sems, recv_sems, w_sems = take(6)

    place = lax.axis_index("ea")
    my_outer = place // TP
    inner = place % TP
    core, x, y = inner % 2, inner // 2 % 2, inner // 4
    slot = core * 4 + y * 2 + x
    x_slot = core * 4 + y * 2 + (1 - x)
    y_slot = core * 4 + (1 - y) * 2 + x
    d_slot = core * 4 + (1 - y) * 2 + (1 - x)
    base = my_outer * TP
    core_dev = base + y * 4 + x * 2 + (1 - core)
    x_dev = base + y * 4 + (1 - x) * 2 + core
    y_dev = base + (1 - y) * 4 + x * 2 + core
    outer_devs = [lax.rem(my_outer + d, outer) * TP + inner for d in range(1, outer)]

    tok_rows, width = tokens.shape
    rows = outer * tok_rows
    cw = width // chunks
    half = w_in.shape[1] // 2

    weight_copies = []
    for k in range(chunks):
        cols = pl.ds(k * cw, cw)
        copy = pltpu.make_async_copy(gate_up.at[0, cols, :], w_in.at[cols, :], w_sems.at[k])
        copy.start()
        weight_copies.append(copy)
    down_copy = pltpu.make_async_copy(down.at[0], w_out, w_sems.at[chunks])
    down_copy.start()

    for k in range(chunks):
        zin[k][my_outer, :, pl.ds(0, cw)] = tokens[:, k * cw : (k + 1) * cw]
    lane = lax.broadcasted_iota(jnp.int32, (tok_rows, LANES), 1)
    gate = jnp.zeros((tok_rows, LANES), F32)
    for j in range(route.shape[1]):
        gate = gate + jnp.where(route[:, j : j + 1] == lane % outer, gates[:, j : j + 1], 0.0)
    high = gate.astype(BF16).astype(F32)
    mid = (gate - high).astype(BF16).astype(F32)
    low = gate - high - mid
    term = lane // outer
    terms = jnp.where(
        term == 0, high, jnp.where(term == 1, mid, jnp.where(term == 2, low, 0.0))
    )
    zin[0][my_outer, :, pl.ds(cw, LANES)] = terms.astype(BF16)

    barrier = pltpu.get_barrier_semaphore()
    peers = [core_dev, x_dev, y_dev] + outer_devs
    for peer in peers:
        pl.semaphore_signal(
            barrier, inc=1, device_id={"ea": peer}, device_id_type=pl.DeviceIdType.MESH
        )
    pl.semaphore_wait(barrier, len(peers))

    sent = []

    def send(src, dst, dev):
        number = len(sent)
        copy = pltpu.make_async_remote_copy(
            src_ref=src,
            dst_ref=dst,
            send_sem=send_sems.at[number],
            recv_sem=recv_sems.at[number],
            device_id={"ea": dev},
            device_id_type=pl.DeviceIdType.MESH,
        )
        copy.start()
        sent.append(copy)
        return copy

    z_copies = []
    for k in range(chunks):
        mine = zin[k].at[my_outer]
        z_copies.append([send(mine, mine, dev) for dev in outer_devs])
    x_in, y_in, core_in, diag_in = {}, {}, {}, {}

    def spread(k):
        for copy in z_copies[k]:
            copy.wait_recv()
        w = zin[k].shape[2]
        xin[k][slot] = zin[k][...].astype(F32).reshape(rows, w).astype(BF16)
        mine = xin[k].at[slot]
        x_in[k] = send(mine, mine, x_dev)
        y_in[k] = send(mine, mine, y_dev)
        core_in[k] = [send(mine, mine, core_dev)]

    def relay(k):
        w = xin[k].shape[2]
        first = w // (2 * LANES) * LANES
        x_in[k].wait_recv()
        a = xin[k].at[x_slot, :, pl.ds(0, first)]
        diag_a = send(a, a, y_dev)
        y_in[k].wait_recv()
        b = xin[k].at[y_slot, :, pl.ds(first, w - first)]
        diag_b = send(b, b, x_dev)
        for s in (x_slot, y_slot):
            core_in[k].append(send(xin[k].at[s], xin[k].at[s], core_dev))
        diag_in[k] = (diag_a, diag_b)

    def relay_diag(k):
        for copy in diag_in[k]:
            copy.wait_recv()
        core_in[k].append(send(xin[k].at[d_slot], xin[k].at[d_slot], core_dev))

    def up(k):
        for copy in core_in[k]:
            copy.wait_recv()
        weight_copies[k].wait()
        value = jnp.dot(
            xin[k][:, :, pl.ds(0, cw)].reshape(TP * rows, cw),
            w_in[pl.ds(k * cw, cw), :],
            preferred_element_type=F32,
        )
        if k == 0:
            both[...] = value
        else:
            both[...] += value

    for t in range(chunks + 3):
        for stage, run in enumerate((spread, relay, relay_diag, up)):
            if 0 <= t - stage < chunks:
                run(t - stage)

    terms = xin[0][:, :, pl.ds(cw, LANES)].reshape(TP * rows, LANES).astype(F32)
    lane = lax.broadcasted_iota(jnp.int32, terms.shape, 1)
    keep = (lane % outer == my_outer) & (lane < 3 * outer)
    gate = jnp.sum(jnp.where(keep, terms, 0.0), axis=1, keepdims=True)
    hidden = (jax.nn.silu(both[:, :half]) * both[:, half:]).astype(BF16)
    down_copy.wait()

    hw = cw // 2
    core_copy, one, two, z_back = {}, {}, {}, {}

    def down_part(k):
        value = jnp.dot(hidden, w_out[:, k * cw : (k + 1) * cw], preferred_element_type=F32) * gate
        part[k][...] = value.astype(BF16).reshape(2, 4, rows, cw)
        core_copy[k] = send(part[k].at[1 - core], from_core[k], core_dev)

    def plane_one(k):
        core_copy[k].wait_recv()
        for yy in range(2):
            for xx in range(2):
                total = part[k][core, 2 * yy + xx].astype(F32) + from_core[k][2 * yy + xx].astype(F32)
                a_sum[k][xx, yy] = total[:, :hw].astype(BF16)
                b_sum[k][yy, xx] = total[:, hw:].astype(BF16)
        one[k] = (
            send(a_sum[k].at[1 - x], a_one[k], x_dev),
            send(b_sum[k].at[1 - y], b_one[k], y_dev),
        )

    def plane_two(k):
        one[k][0].wait_recv()
        a_mid[k][...] = (a_sum[k][x].astype(F32) + a_one[k][...].astype(F32)).astype(BF16)
        to_y = send(a_mid[k].at[1 - y], a_two[k], y_dev)
        one[k][1].wait_recv()
        b_mid[k][...] = (b_sum[k][y].astype(F32) + b_one[k][...].astype(F32)).astype(BF16)
        two[k] = (to_y, send(b_mid[k].at[1 - x], b_two[k], x_dev))

    def outer_send(k):
        two[k][0].wait_recv()
        a = a_mid[k][y].astype(F32) + a_two[k][...].astype(F32)
        z_send[k][:, :, pl.ds(0, hw)] = a.reshape(outer, tok_rows, hw).astype(BF16)
        two[k][1].wait_recv()
        b = b_mid[k][x].astype(F32) + b_two[k][...].astype(F32)
        z_send[k][:, :, pl.ds(hw, hw)] = b.reshape(outer, tok_rows, hw).astype(BF16)
        z_back[k] = [
            send(z_send[k].at[lax.rem(my_outer + d, outer)], z_recv[k].at[d - 1], outer_devs[d - 1])
            for d in range(1, outer)
        ]

    def finish(k):
        total = z_send[k][my_outer].astype(F32)
        for d, copy in enumerate(z_back[k]):
            copy.wait_recv()
            total = total + z_recv[k][d].astype(F32)
        out[:, k * cw : (k + 1) * cw] = total.astype(BF16)

    for t in range(chunks + 4):
        for stage, run in enumerate((down_part, plane_one, plane_two, outer_send, finish)):
            if 0 <= t - stage < chunks:
                run(t - stage)

    for copy in sent:
        copy.wait_send()


def local(tokens, route_slot, gates, gate_up, down):
    tok_rows, width = tokens.shape
    outer = lax.axis_size("ea") // TP
    chunks = chunk_count(width)
    rows = outer * tok_rows
    cw = width // chunks
    hw = cw // 2
    wide = [cw + LANES] + [cw] * (chunks - 1)
    each = lambda *shape: [pltpu.VMEM(shape, BF16)] * chunks
    copies = copies_per_launch(outer, chunks)
    scratch = (
        [pltpu.VMEM((outer, tok_rows, w), BF16) for w in wide]
        + [pltpu.VMEM((TP, rows, w), BF16) for w in wide]
        + each(2, 4, rows, cw)
        + each(4, rows, cw)
        + each(2, 2, rows, hw) * 2
        + each(2, rows, hw) * 4
        + each(rows, hw) * 2
        + each(outer, tok_rows, cw)
        + each(outer - 1, tok_rows, cw)
        + [
            pltpu.VMEM(gate_up.shape[1:], BF16),
            pltpu.VMEM(down.shape[1:], BF16),
            pltpu.VMEM((TP * rows, gate_up.shape[2]), F32),
            pltpu.SemaphoreType.DMA((copies,)),
            pltpu.SemaphoreType.DMA((copies,)),
            pltpu.SemaphoreType.DMA((chunks + 1,)),
        ]
    )
    vmem = pl.BlockSpec(memory_space=pltpu.VMEM)
    hbm = pl.BlockSpec(memory_space=pl.ANY)
    return pl.pallas_call(
        functools.partial(kernel, outer, chunks),
        out_shape=jax.ShapeDtypeStruct((tok_rows, width), BF16),
        in_specs=[vmem, vmem, vmem, hbm, hbm],
        out_specs=vmem,
        scratch_shapes=scratch,
        compiler_params=pltpu.CompilerParams(
            collective_id=0, has_side_effects=True, vmem_limit_bytes=60000 * 1024
        ),
    )(tokens, route_slot, gates, gate_up, down)


def solution(mesh):
    placed = (
        P(("ga", "ea"), None),
        P(("ga", "ea"), None),
        P(("ga", "ea"), None),
        P("ea", None, None),
        P("ea", None, None),
    )
    return jax.shard_map(
        local, mesh=mesh, in_specs=placed, out_specs=P(("ga", "ea"), None), check_vma=False
    )
```

```python
import functools

import jax
import jax.numpy as jnp
from jax import lax
from jax.experimental import pallas as pl
from jax.experimental.pallas import tpu as pltpu
from jax.sharding import PartitionSpec as P

TP = 8
LANES = 128
F32 = jnp.float32
BF16 = jnp.bfloat16


def copies_per_launch(outer):
    return outer * (8 + 5) + 2 * (outer - 1)


def nearest(place, count, order):
    above = count - 1 - place
    pairs = jnp.minimum(place, above)
    step = (order + 1) // 2
    near = place + (step if order % 2 else -step)
    far = jnp.where(place < above, place + (order - pairs), place - (order - pairs))
    return jnp.where(order <= 2 * pairs, near, far)


def column(row, count):
    down = lax.broadcasted_iota(jnp.int32, (count, count), 0)
    across = lax.broadcasted_iota(jnp.int32, (count, count), 1)
    return jnp.sum(jnp.where(down == across, row, 0.0), axis=1, keepdims=True)


def kernel(outer, tile, schedule, *refs):
    tokens, route, gates, gate_up, down, out = refs[:6]
    xin, part, from_core, a_sum, b_sum, a_one, b_one, a_mid, b_mid, a_two, b_two = refs[6:17]
    z_send, z_recv, w_in, w_out, hidden, weight, send_sems, recv_sems, w_sems = refs[17:]

    place = lax.axis_index("ea")
    my_outer = place // TP
    inner = place % TP
    core, x, y = inner % 2, inner // 2 % 2, inner // 4
    slot = core * 4 + y * 2 + x
    x_slot = core * 4 + y * 2 + (1 - x)
    y_slot = core * 4 + (1 - y) * 2 + x
    d_slot = core * 4 + (1 - y) * 2 + (1 - x)
    base = my_outer * TP
    core_dev = base + y * 4 + x * 2 + (1 - core)
    x_dev = base + y * 4 + (1 - x) * 2 + core
    y_dev = base + (1 - y) * 4 + x * 2 + core
    near = [nearest(my_outer, outer, i) if i else my_outer for i in range(outer)]
    outer_devs = [o * TP + inner for o in near]

    tok_rows, width = tokens.shape
    rows = TP * tok_rows
    half = w_in.shape[1] // 2
    left = width // (2 * LANES) * LANES
    right = width - left

    in_copy = pltpu.make_async_copy(gate_up.at[0], w_in, w_sems.at[0])
    in_copy.start()
    down_copy = pltpu.make_async_copy(down.at[0], w_out, w_sems.at[1])
    down_copy.start()

    xin[my_outer, slot, :, pl.ds(0, width)] = tokens[...]
    lane = lax.broadcasted_iota(jnp.int32, (tok_rows, LANES), 1)
    gate = jnp.zeros((tok_rows, LANES), F32)
    for j in range(route.shape[0]):
        chosen = column(route[j : j + 1, :].astype(F32), tok_rows)
        value = column(gates[j : j + 1, :], tok_rows)
        gate = gate + jnp.where(chosen == (lane % outer).astype(F32), value, 0.0)
    high = gate.astype(BF16).astype(F32)
    mid = (gate - high).astype(BF16).astype(F32)
    low = gate - high - mid
    term = lane // outer
    terms = jnp.where(
        term == 0, high, jnp.where(term == 1, mid, jnp.where(term == 2, low, 0.0))
    )
    xin[my_outer, slot, :, pl.ds(width, LANES)] = terms.astype(BF16)

    barrier = pltpu.get_barrier_semaphore()
    peers = [core_dev, x_dev, y_dev] + outer_devs[1:]
    for peer in peers:
        pl.semaphore_signal(
            barrier, inc=1, device_id={"ea": peer}, device_id_type=pl.DeviceIdType.MESH
        )
    pl.semaphore_wait(barrier, len(peers))

    sent = []
    fixed = 2 * outer

    def remote(src, dst, dev, arrival):
        copy = pltpu.make_async_remote_copy(
            src_ref=src,
            dst_ref=dst,
            send_sem=send_sems.at[len(sent)],
            recv_sem=recv_sems.at[arrival],
            device_id={"ea": dev},
            device_id_type=pl.DeviceIdType.MESH,
        )
        copy.start()
        sent.append(copy)
        return copy

    def send(src, dst, dev):
        return remote(src, dst, dev, fixed + len(sent))

    def arrived(ref, number):
        pltpu.make_async_remote_copy(
            src_ref=ref,
            dst_ref=ref,
            send_sem=send_sems.at[0],
            recv_sem=recv_sems.at[number],
            device_id={"ea": core_dev},
            device_id_type=pl.DeviceIdType.MESH,
        ).wait_recv()

    mine = xin.at[my_outer, slot]
    x_in, y_in, core_in, diag_in = {}, {}, {}, {}

    def spread(i):
        block = xin.at[near[i], slot]
        if i:
            arrived(block, near[i])
        x_in[i] = send(block, block, x_dev)
        y_in[i] = send(block, block, y_dev)
        core_in[i] = [send(block, block, core_dev)]
        if i == 0:
            for dev in outer_devs[1:]:
                remote(mine, mine, dev, my_outer)

    def relay(i):
        o = near[i]
        first = (width + LANES) // (2 * LANES) * LANES
        x_in[i].wait_recv()
        a = xin.at[o, x_slot, :, pl.ds(0, first)]
        diag_a = send(a, a, y_dev)
        y_in[i].wait_recv()
        b = xin.at[o, y_slot, :, pl.ds(first, width + LANES - first)]
        diag_b = send(b, b, x_dev)
        for s in (x_slot, y_slot):
            core_in[i].append(send(xin.at[o, s], xin.at[o, s], core_dev))
        diag_in[i] = (diag_a, diag_b)

    def relay_diag(i):
        for copy in diag_in[i]:
            copy.wait_recv()
        block = xin.at[near[i], d_slot]
        core_in[i].append(send(block, block, core_dev))

    def up(i):
        for copy in core_in[i]:
            copy.wait_recv()
        if i == 0:
            in_copy.wait()
        o = near[i]
        both = jnp.zeros((rows, 2 * half), F32)
        for at in range(0, width, tile):
            value = xin[o, :, :, pl.ds(at, tile)].astype(F32).reshape(rows, tile).astype(BF16)
            both = both + jnp.dot(value, w_in[at : at + tile, :], preferred_element_type=F32)
        hidden[i] = (jax.nn.silu(both[:, :half]) * both[:, half:]).astype(BF16)
        terms = xin[o, :, :, pl.ds(width, LANES)].astype(F32).reshape(rows, LANES)
        lane = lax.broadcasted_iota(jnp.int32, terms.shape, 1)
        keep = (lane % outer == my_outer) & (lane < 3 * outer)
        gate = jnp.sum(jnp.where(keep, terms, 0.0), axis=1, keepdims=True)
        weight[i] = jnp.broadcast_to(gate, (rows, LANES))

    core_copy, one, two = {}, {}, {}
    ready = []

    def down_part(i):
        if not ready:
            down_copy.wait()
            ready.append(True)
        gate = weight[i][:, :1]
        for at in range(0, width, tile):
            value = jnp.dot(
                hidden[i], w_out[:, at : at + tile], preferred_element_type=F32
            ) * gate
            part[i, :, :, :, pl.ds(at, tile)] = value.reshape(2, 4, tok_rows, tile).astype(BF16)
        core_copy[i] = send(part.at[i, 1 - core], from_core.at[i], core_dev)

    def plane_one(i):
        core_copy[i].wait_recv()
        for yy in range(2):
            for xx in range(2):
                place = 2 * yy + xx
                total = part[i, core, place].astype(F32) + from_core[i, place].astype(F32)
                a_sum[i, xx, yy] = total[:, :left].astype(BF16)
                b_sum[i, yy, xx] = total[:, left:].astype(BF16)
        one[i] = (
            send(a_sum.at[i, 1 - x], a_one.at[i], x_dev),
            send(b_sum.at[i, 1 - y], b_one.at[i], y_dev),
        )

    def plane_two(i):
        one[i][0].wait_recv()
        a_mid[i] = (a_sum[i, x].astype(F32) + a_one[i].astype(F32)).astype(BF16)
        to_y = send(a_mid.at[i, 1 - y], a_two.at[i], y_dev)
        one[i][1].wait_recv()
        b_mid[i] = (b_sum[i, y].astype(F32) + b_one[i].astype(F32)).astype(BF16)
        two[i] = (to_y, send(b_mid.at[i, 1 - x], b_two.at[i], x_dev))

    def outer_send(i):
        two[i][0].wait_recv()
        a = a_mid[i, y].astype(F32) + a_two[i].astype(F32)
        two[i][1].wait_recv()
        b = b_mid[i, x].astype(F32) + b_two[i].astype(F32)
        if i:
            z_send[i - 1, :, pl.ds(0, left)] = a.astype(BF16)
            z_send[i - 1, :, pl.ds(left, right)] = b.astype(BF16)
            remote(z_send.at[i - 1], z_recv.at[my_outer], outer_devs[i], outer + my_outer)
        else:
            for j in range(1, outer):
                arrived(z_recv.at[near[j]], outer + near[j])
                a = a + z_recv[near[j], :, pl.ds(0, left)].astype(F32)
                b = b + z_recv[near[j], :, pl.ds(left, right)].astype(F32)
            out[:, :left] = a.astype(BF16)
            out[:, left:] = b.astype(BF16)

    stages = {
        "A": spread,
        "B": relay,
        "C": relay_diag,
        "D": up,
        "P": down_part,
        "Q": plane_one,
        "R": plane_two,
        "S": outer_send,
    }
    for name, i in schedule:
        stages[name](i)
    for copy in sent:
        copy.wait_send()


def staged(names, order):
    steps = []
    for t in range(len(order) + len(names) - 1):
        for stage, name in enumerate(names):
            if 0 <= t - stage < len(order):
                steps.append((name, order[t - stage]))
    return steps


def plan(outer):
    order = list(range(outer))
    return staged("ABCD", order) + staged("PQRS", order[::-1])


def local(tokens, route_slot, gates, gate_up, down):
    tok_rows, width = tokens.shape
    outer = lax.axis_size("ea") // TP
    tile = next(t for t in (1024, 512, 256, 128) if width % t == 0)
    left = width // (2 * LANES) * LANES
    right = width - left
    rows = TP * tok_rows
    buf = lambda *shape: pltpu.VMEM(shape, BF16)
    copies = copies_per_launch(outer)
    scratch = [
        buf(outer, TP, tok_rows, width + LANES),
        buf(outer, 2, 4, tok_rows, width),
        buf(outer, 4, tok_rows, width),
        buf(outer, 2, 2, tok_rows, left),
        buf(outer, 2, 2, tok_rows, right),
        buf(outer, 2, tok_rows, left),
        buf(outer, 2, tok_rows, right),
        buf(outer, 2, tok_rows, left),
        buf(outer, 2, tok_rows, right),
        buf(outer, tok_rows, left),
        buf(outer, tok_rows, right),
        buf(max(outer - 1, 1), tok_rows, width),
        buf(outer, tok_rows, width),
        pltpu.VMEM(gate_up.shape[1:], BF16),
        pltpu.VMEM(down.shape[1:], BF16),
        buf(outer, rows, gate_up.shape[2] // 2),
        pltpu.VMEM((outer, rows, LANES), F32),
        pltpu.SemaphoreType.DMA((copies,)),
        pltpu.SemaphoreType.DMA((copies + 2 * outer,)),
        pltpu.SemaphoreType.DMA((2,)),
    ]
    vmem = pl.BlockSpec(memory_space=pltpu.VMEM)
    hbm = pl.BlockSpec(memory_space=pl.ANY)
    return pl.pallas_call(
        functools.partial(kernel, outer, tile, plan(outer)),
        out_shape=jax.ShapeDtypeStruct((tok_rows, width), BF16),
        in_specs=[vmem, vmem, vmem, hbm, hbm],
        out_specs=vmem,
        scratch_shapes=scratch,
        compiler_params=pltpu.CompilerParams(
            collective_id=0, has_side_effects=True, vmem_limit_bytes=60000 * 1024
        ),
    )(tokens, route_slot.T, gates.T, gate_up, down)


def solution(mesh):
    placed = (
        P(("ga", "ea"), None),
        P(("ga", "ea"), None),
        P(("ga", "ea"), None),
        P("ea", None, None),
        P("ea", None, None),
    )
    return jax.shard_map(
        local, mesh=mesh, in_specs=placed, out_specs=P(("ga", "ea"), None), check_vma=False
    )
```

```python
import functools

import jax
import jax.numpy as jnp
from jax import lax
from jax.experimental import pallas as pl
from jax.experimental.pallas import tpu as pltpu
from jax.sharding import PartitionSpec as P

TP = 8
LANES = 128
F32 = jnp.float32
BF16 = jnp.bfloat16


def copies_per_launch(outer):
    return outer * (8 + 6) + 2 * (outer - 1)


def nearest(place, count, order):
    above = count - 1 - place
    pairs = jnp.minimum(place, above)
    step = (order + 1) // 2
    near = place + (step if order % 2 else -step)
    far = jnp.where(place < above, place + (order - pairs), place - (order - pairs))
    return jnp.where(order <= 2 * pairs, near, far)


def column(row, count):
    down = lax.broadcasted_iota(jnp.int32, (count, count), 0)
    across = lax.broadcasted_iota(jnp.int32, (count, count), 1)
    return jnp.sum(jnp.where(down == across, row, 0.0), axis=1, keepdims=True)


def kernel(outer, tile, schedule, *refs):
    tokens, route, gates, gate_up, down, out = refs[:6]
    xin, part, from_core, a_sum, b_sum, a_one, b_one, a_mid, b_mid, a_two, b_two = refs[6:17]
    z_send, z_recv, w_in, w_out, hidden, weight, route_in, gates_in = refs[17:25]
    send_sems, recv_sems, w_sems = refs[25:]

    place = lax.axis_index("ea")
    my_outer = place // TP
    inner = place % TP
    core, x, y = inner % 2, inner // 2 % 2, inner // 4
    slot = core * 4 + y * 2 + x
    x_slot = core * 4 + y * 2 + (1 - x)
    y_slot = core * 4 + (1 - y) * 2 + x
    d_slot = core * 4 + (1 - y) * 2 + (1 - x)
    base = my_outer * TP
    core_dev = base + y * 4 + x * 2 + (1 - core)
    x_dev = base + y * 4 + (1 - x) * 2 + core
    y_dev = base + (1 - y) * 4 + x * 2 + core
    near = [nearest(my_outer, outer, i) if i else my_outer for i in range(outer)]
    outer_devs = [o * TP + inner for o in near]

    barrier = pltpu.get_barrier_semaphore()
    peers = [core_dev, x_dev, y_dev] + outer_devs[1:]
    for peer in peers:
        pl.semaphore_signal(
            barrier, inc=1, device_id={"ea": peer}, device_id_type=pl.DeviceIdType.MESH
        )

    tok_rows, width = tokens.shape
    mine = xin.at[my_outer, slot]
    small = [
        pltpu.make_async_copy(tokens, mine.at[:, pl.ds(0, width)], w_sems.at[2]),
        pltpu.make_async_copy(route, route_in, w_sems.at[3]),
        pltpu.make_async_copy(gates, gates_in, w_sems.at[4]),
    ]
    for copy in small:
        copy.start()
    rows = TP * tok_rows
    half = w_in.shape[1] // 2
    left = width // (2 * LANES) * LANES
    right = width - left

    in_copy = pltpu.make_async_copy(gate_up.at[0], w_in, w_sems.at[0])
    in_copy.start()
    down_copy = pltpu.make_async_copy(down.at[0], w_out, w_sems.at[1])
    down_copy.start()

    small[1].wait()
    small[2].wait()
    lane = lax.broadcasted_iota(jnp.int32, (tok_rows, LANES), 1)
    gate = jnp.zeros((tok_rows, LANES), F32)
    for j in range(route.shape[0]):
        chosen = column(route_in[j : j + 1, :].astype(F32), tok_rows)
        value = column(gates_in[j : j + 1, :], tok_rows)
        gate = gate + jnp.where(chosen == (lane % outer).astype(F32), value, 0.0)
    high = gate.astype(BF16).astype(F32)
    mid = (gate - high).astype(BF16).astype(F32)
    low = gate - high - mid
    term = lane // outer
    terms = jnp.where(
        term == 0, high, jnp.where(term == 1, mid, jnp.where(term == 2, low, 0.0))
    )
    xin[my_outer, slot, :, pl.ds(width, LANES)] = terms.astype(BF16)

    small[0].wait()
    pl.semaphore_wait(barrier, len(peers))

    sent = []
    fixed = 2 * outer

    def remote(src, dst, dev, arrival):
        copy = pltpu.make_async_remote_copy(
            src_ref=src,
            dst_ref=dst,
            send_sem=send_sems.at[len(sent)],
            recv_sem=recv_sems.at[arrival],
            device_id={"ea": dev},
            device_id_type=pl.DeviceIdType.MESH,
        )
        copy.start()
        sent.append(copy)
        return copy

    def send(src, dst, dev):
        return remote(src, dst, dev, fixed + len(sent))

    def arrived(ref, number):
        pltpu.make_async_remote_copy(
            src_ref=ref,
            dst_ref=ref,
            send_sem=send_sems.at[0],
            recv_sem=recv_sems.at[number],
            device_id={"ea": core_dev},
            device_id_type=pl.DeviceIdType.MESH,
        ).wait_recv()

    x_in, y_in, core_in, diag_in = {}, {}, {}, {}

    def spread(i):
        block = xin.at[near[i], slot]
        if i:
            arrived(block, near[i])
        x_in[i] = send(block, block, x_dev)
        y_in[i] = send(block, block, y_dev)
        core_in[i] = [send(block, block, core_dev)]
        if i == 0:
            for dev in outer_devs[1:]:
                remote(mine, mine, dev, my_outer)

    def relay(i):
        o = near[i]
        first = (width + LANES) // (2 * LANES) * LANES
        x_in[i].wait_recv()
        a = xin.at[o, x_slot, :, pl.ds(0, first)]
        diag_a = send(a, a, y_dev)
        y_in[i].wait_recv()
        b = xin.at[o, y_slot, :, pl.ds(first, width + LANES - first)]
        diag_b = send(b, b, x_dev)
        for s in (x_slot, y_slot):
            core_in[i].append(send(xin.at[o, s], xin.at[o, s], core_dev))
        diag_in[i] = (diag_a, diag_b)

    def relay_diag(i):
        for copy in diag_in[i]:
            copy.wait_recv()
        block = xin.at[near[i], d_slot]
        core_in[i].append(send(block, block, core_dev))

    def up(i):
        for copy in core_in[i]:
            copy.wait_recv()
        if i == 0:
            in_copy.wait()
        o = near[i]
        both = jnp.zeros((rows, 2 * half), F32)
        for at in range(0, width, tile):
            value = xin[o, :, :, pl.ds(at, tile)].astype(F32).reshape(rows, tile).astype(BF16)
            both = both + jnp.dot(value, w_in[at : at + tile, :], preferred_element_type=F32)
        hidden[i] = (jax.nn.silu(both[:, :half]) * both[:, half:]).astype(BF16)
        terms = xin[o, :, :, pl.ds(width, LANES)].astype(F32).reshape(rows, LANES)
        lane = lax.broadcasted_iota(jnp.int32, terms.shape, 1)
        keep = (lane % outer == my_outer) & (lane < 3 * outer)
        gate = jnp.sum(jnp.where(keep, terms, 0.0), axis=1, keepdims=True)
        weight[i] = jnp.broadcast_to(gate, (rows, LANES))

    core_copy, one, two = {}, {}, {}
    ready = []

    def down_part(i):
        if not ready:
            down_copy.wait()
            ready.append(True)
        gate = weight[i][:, :1]
        core_copy[i] = []
        for at in range(0, width, tile):
            value = jnp.dot(
                hidden[i], w_out[:, at : at + tile], preferred_element_type=F32
            ) * gate
            part[i, :, :, :, pl.ds(at, tile)] = value.reshape(2, 4, tok_rows, tile).astype(BF16)
            for begin, count in ((0, left), (left, right)):
                if at + tile == begin + count:
                    cols = pl.ds(begin, count)
                    core_copy[i].append(
                        send(
                            part.at[i, 1 - core, :, :, cols],
                            from_core.at[i, :, :, cols],
                            core_dev,
                        )
                    )

    def plane_one(i):
        core_copy[i][0].wait_recv()
        cols = pl.ds(0, left)
        for yy in range(2):
            for xx in range(2):
                own = part[i, core, 2 * yy + xx, :, cols].astype(F32)
                a_sum[i, xx, yy] = (own + from_core[i, 2 * yy + xx, :, cols].astype(F32)).astype(BF16)
        to_x = send(a_sum.at[i, 1 - x], a_one.at[i], x_dev)
        core_copy[i][1].wait_recv()
        cols = pl.ds(left, right)
        for yy in range(2):
            for xx in range(2):
                own = part[i, core, 2 * yy + xx, :, cols].astype(F32)
                b_sum[i, yy, xx] = (own + from_core[i, 2 * yy + xx, :, cols].astype(F32)).astype(BF16)
        one[i] = (to_x, send(b_sum.at[i, 1 - y], b_one.at[i], y_dev))

    def plane_two(i):
        one[i][0].wait_recv()
        a_mid[i] = (a_sum[i, x].astype(F32) + a_one[i].astype(F32)).astype(BF16)
        to_y = send(a_mid.at[i, 1 - y], a_two.at[i], y_dev)
        one[i][1].wait_recv()
        b_mid[i] = (b_sum[i, y].astype(F32) + b_one[i].astype(F32)).astype(BF16)
        two[i] = (to_y, send(b_mid.at[i, 1 - x], b_two.at[i], x_dev))

    def outer_send(i):
        two[i][0].wait_recv()
        a = a_mid[i, y].astype(F32) + a_two[i].astype(F32)
        two[i][1].wait_recv()
        b = b_mid[i, x].astype(F32) + b_two[i].astype(F32)
        if i:
            z_send[i - 1, :, pl.ds(0, left)] = a.astype(BF16)
            z_send[i - 1, :, pl.ds(left, right)] = b.astype(BF16)
            remote(z_send.at[i - 1], z_recv.at[my_outer], outer_devs[i], outer + my_outer)
        else:
            for j in range(1, outer):
                arrived(z_recv.at[near[j]], outer + near[j])
                a = a + z_recv[near[j], :, pl.ds(0, left)].astype(F32)
                b = b + z_recv[near[j], :, pl.ds(left, right)].astype(F32)
            out[:, :left] = a.astype(BF16)
            out[:, left:] = b.astype(BF16)

    stages = {
        "A": spread,
        "B": relay,
        "C": relay_diag,
        "D": up,
        "P": down_part,
        "Q": plane_one,
        "R": plane_two,
        "S": outer_send,
    }
    for name, i in schedule:
        stages[name](i)
    for copy in sent:
        copy.wait_send()


def staged(names, order):
    steps = []
    for t in range(len(order) + len(names) - 1):
        for stage, name in enumerate(names):
            if 0 <= t - stage < len(order):
                steps.append((name, order[t - stage]))
    return steps


def plan(outer):
    order = list(range(outer))
    return staged("ABCD", order) + staged("PQRS", order[::-1])


def local(tokens, route_slot, gates, gate_up, down):
    tok_rows, width = tokens.shape
    outer = lax.axis_size("ea") // TP
    left = width // (2 * LANES) * LANES
    right = width - left
    tile = next(t for t in (512, 256, 128) if left % t == 0 and right % t == 0)
    rows = TP * tok_rows
    buf = lambda *shape: pltpu.VMEM(shape, BF16)
    copies = copies_per_launch(outer)
    scratch = [
        buf(outer, TP, tok_rows, width + LANES),
        buf(outer, 2, 4, tok_rows, width),
        buf(outer, 4, tok_rows, width),
        buf(outer, 2, 2, tok_rows, left),
        buf(outer, 2, 2, tok_rows, right),
        buf(outer, 2, tok_rows, left),
        buf(outer, 2, tok_rows, right),
        buf(outer, 2, tok_rows, left),
        buf(outer, 2, tok_rows, right),
        buf(outer, tok_rows, left),
        buf(outer, tok_rows, right),
        buf(max(outer - 1, 1), tok_rows, width),
        buf(outer, tok_rows, width),
        pltpu.VMEM(gate_up.shape[1:], BF16),
        pltpu.VMEM(down.shape[1:], BF16),
        buf(outer, rows, gate_up.shape[2] // 2),
        pltpu.VMEM((outer, rows, LANES), F32),
        pltpu.VMEM(route_slot.shape[::-1], route_slot.dtype),
        pltpu.VMEM(gates.shape[::-1], gates.dtype),
        pltpu.SemaphoreType.DMA((copies,)),
        pltpu.SemaphoreType.DMA((copies + 2 * outer,)),
        pltpu.SemaphoreType.DMA((5,)),
    ]
    vmem = pl.BlockSpec(memory_space=pltpu.VMEM)
    hbm = pl.BlockSpec(memory_space=pl.ANY)
    return pl.pallas_call(
        functools.partial(kernel, outer, tile, plan(outer)),
        out_shape=jax.ShapeDtypeStruct((tok_rows, width), BF16),
        in_specs=[hbm] * 5,
        out_specs=vmem,
        scratch_shapes=scratch,
        compiler_params=pltpu.CompilerParams(
            collective_id=0, has_side_effects=True, vmem_limit_bytes=60000 * 1024
        ),
    )(tokens, route_slot.T, gates.T, gate_up, down)


def solution(mesh):
    placed = (
        P(("ga", "ea"), None),
        P(("ga", "ea"), None),
        P(("ga", "ea"), None),
        P("ea", None, None),
        P("ea", None, None),
    )
    return jax.shard_map(
        local, mesh=mesh, in_specs=placed, out_specs=P(("ga", "ea"), None), check_vma=False
    )
```
